32 devices in a mesh: section: 16 (over z, y, core), dp: 2 (over x).
Axes of the slice: x: 2, y: 2, z: 4, core: 2. Of those that a mesh axis runs over, the one named last changes fastest.
Arguments:
- layer_in: bfloat16 [16, 256, 5120], P('section', 'dp'), may hold values from -6 to 6
- latent: bfloat16 [16, 256, 384], P('section', 'dp'), may hold values from -6 to 6
- mix_grad: bfloat16 [16, 256, 5120], P('section', 'dp'), may hold values from -0.375 to 0.375
- down_proj: bfloat16 [16, 5120, 384], P('section', 'dp'), may hold values from -0.078125 to 0.078125
- up_proj: bfloat16 [16, 384, 5120], P('section', None, 'dp'), may hold values from -0.3125 to 0.3125
- norm_gain: bfloat16 [16, 5120], P('section', 'dp'), may hold values from 0.5 to 1.5
- mix_weight: float32 [16, 8], P('section'), may hold values from 0.2 to 1
Outputs:
- up_grad: bfloat16 [16, 384, 5120], P('section', None, 'dp')
- down_grad: bfloat16 [16, 5120, 384], P('section', 'dp')
- gain_grad: float32 [16, 5120], P('section', 'dp')
- mixing_grad: float32 [16, 8], P('section')
The draws below stay inside these ranges and needn't reach their ends.
All inputs are finite; a program needn't handle non-finite values.
Results may differ from the reference program's by a relative error of at most 0.0064.
Values may be sent and summed in bfloat16 or wider, within the bound.
A program may use at most 128 MiB of HBM per device.

```python
import jax
import jax.numpy as jnp
from jax import lax

D = 5120
R = 384
MIXES = 8
LAYERS = 16
TOKENS = 256


def steps_of(stream_key, dims, cuts, least, largest):
    def one(axis_at, blocks):
        steps = jax.random.uniform(jax.random.fold_in(jax.random.fold_in(stream_key, 6), axis_at), (blocks,), jnp.float32, least / len(cuts), largest / len(cuts))
        return jnp.repeat(jnp.exp(steps), dims[axis_at] // blocks).reshape((-1,) + (1,) * (len(dims) - axis_at - 1))

    level = one(*cuts[0])
    for cut in cuts[1:]:
        level = level * one(*cut)
    return level


def gaussian(stream_key, extent, scale, bound, split=(), held_as=jnp.bfloat16):
    loudness = steps_of(stream_key, extent, split, -0.22, 0.18) if split else 1.0
    array = jax.random.normal(stream_key, extent, jnp.float32) * scale * loudness
    return jnp.minimum(jnp.maximum(array, -bound), bound).astype(held_as)


def setup_inputs(seed: int = 0) -> dict:
    arg_keys = jax.random.split(jax.random.key(seed), 8)
    layer_in = gaussian(arg_keys[0], (LAYERS, TOKENS, D), 1.0, 6.0, ((0, 16), (1, 2)))
    latent = gaussian(arg_keys[1], (LAYERS, TOKENS, R), 1.0, 6.0, ((0, 16), (1, 2)))
    mix_grad = gaussian(arg_keys[2], (LAYERS, TOKENS, D), (TOKENS ** -0.5), 0.375, ((0, 16), (1, 2)))
    down_proj = gaussian(arg_keys[3], (LAYERS, D, R), D ** -0.5, 0.078125, ((0, 16), (1, 2)))
    up_proj = gaussian(arg_keys[4], (LAYERS, R, D), R ** -0.5, 0.3125, ((0, 16), (2, 2)))
    norm_gain = jnp.clip(1.0 + 0.1 * jax.random.normal(arg_keys[5], (LAYERS, D), jnp.float32), 0.5, 1.5).astype(jnp.bfloat16)
    mix_weight = jnp.clip(0.2 + 0.8 * jax.random.uniform(arg_keys[6], (LAYERS, MIXES), jnp.float32) ** steps_of(arg_keys[6], (LAYERS, MIXES), ((0, 16),), -0.2, 0.2), 0.2, 1.0)
    return {"layer_in": layer_in, "latent": latent, "mix_grad": mix_grad, "down_proj": down_proj, "up_proj": up_proj, "norm_gain": norm_gain, "mix_weight": mix_weight}


epsilon = 1e-06
root_coef = 0.7978845608028654

def gelu_pair(values):
    tangent = jnp.tanh(root_coef * (values + 0.044715 * values * values * values))
    result = 0.5 * values * (1.0 + tangent)
    slopes = 0.5 * (1.0 + tangent) + 0.5 * values * (1.0 - tangent * tangent) * root_coef * (1.0 + 3.0 * 0.044715 * values * values)
    return (result, slopes)

def reference(layer_in, latent, mix_grad, down_proj, up_proj, norm_gain, mix_weight):
    stride = LAYERS // MIXES

    def one_section(index):
        inputs = lax.dynamic_index_in_dim(layer_in, index, 0, False).astype(jnp.float32)
        mean_sq = lax.optimization_barrier(jnp.mean(inputs * inputs, axis=1, keepdims=True))
        inv_rms = lax.rsqrt(mean_sq + epsilon)
        scaled = inputs * inv_rms
        gain_row = lax.dynamic_index_in_dim(norm_gain, index, 0, False).astype(jnp.float32)
        normed = (scaled * gain_row).astype(jnp.bfloat16)
        latent_row = lax.dynamic_index_in_dim(latent, index, 0, False).astype(jnp.float32)
        activated, slopes = gelu_pair(latent_row)
        act_half = activated.astype(jnp.bfloat16)
        up_block = lax.dynamic_index_in_dim(up_proj, index, 0, False)
        down_block = lax.dynamic_index_in_dim(down_proj, index, 0, False)
        layer_out = inputs + jnp.dot(act_half, up_block, preferred_element_type=jnp.float32)
        weight_row = lax.dynamic_index_in_dim(mix_weight, index, 0, False)
        grad_sum = jnp.zeros(inputs.shape, jnp.float32)
        products = []
        for member in range(MIXES):
            target = index + member * stride
            inside = (target < LAYERS).astype(jnp.float32)
            clamped = jnp.minimum(target, LAYERS - 1).astype(jnp.int32)
            piece = lax.dynamic_index_in_dim(mix_grad, clamped, 0, False).astype(jnp.float32) * inside
            products.append(jnp.sum(piece * layer_out))
            grad_sum = grad_sum + weight_row[member] * piece
        grad_half = grad_sum.astype(jnp.bfloat16)
        act_grad = jnp.dot(grad_half, up_block.T, preferred_element_type=jnp.float32)
        latent_grad = (act_grad * slopes).astype(jnp.bfloat16)
        up_grad = jnp.dot(act_half.T, grad_half, preferred_element_type=jnp.float32).astype(jnp.bfloat16)
        down_grad = jnp.dot(normed.T, latent_grad, preferred_element_type=jnp.float32).astype(jnp.bfloat16)
        norm_grad = jnp.dot(latent_grad, down_block.T, preferred_element_type=jnp.float32)
        gain_grad = lax.optimization_barrier(jnp.sum(norm_grad * scaled, axis=0))
        return (up_grad, down_grad, gain_grad, jnp.stack(products))
    up_grad, down_grad, gain_grad, mixing_grad = lax.map(one_section, jnp.arange(LAYERS, dtype=jnp.int32))
    return (up_grad, down_grad, gain_grad, mixing_grad)
```

```python
import functools

import jax
import jax.numpy as jnp
from jax import lax
from jax.experimental import pallas as pl
from jax.experimental.pallas import tpu as pltpu
from jax.sharding import PartitionSpec as P

MIXES = 8
LEVELS = MIXES // 2
SLOTS = 6
CHUNK = 16
TILE = 640

epsilon = 1e-06
root_coef = 0.7978845608028654
MESH = pl.DeviceIdType.MESH
F32 = jnp.float32
BF16 = jnp.bfloat16
DMA = pltpu.SemaphoreType.DMA


def gelu_pair(values):
    tangent = jnp.tanh(root_coef * (values + 0.044715 * values * values * values))
    result = 0.5 * values * (1.0 + tangent)
    slopes = 0.5 * (1.0 + tangent) + 0.5 * values * (1.0 - tangent * tangent) * root_coef * (
        1.0 + 3.0 * 0.044715 * values * values
    )
    return (result, slopes)


def fold(values):
    rows, cols = values.shape
    total = jnp.sum(values.reshape(rows // 8, 8, cols), axis=0)
    out = total[:, 0:128]
    for at in range(128, cols, 128):
        out = out + total[:, at : at + 128]
    return out


def rows(start, size, unit):
    return pl.ds(pl.multiple_of(start, unit), size)


def scratch(n, own_rows, width, latents):
    feats = width // n
    tokens = own_rows * n
    half = tokens // 2
    chunks = half // CHUNK
    return dict(
        xo=pltpu.VMEM((own_rows, width), BF16),
        cin=pltpu.VMEM((tokens, feats), BF16),
        latv=pltpu.VMEM((tokens, latents), BF16),
        gb=pltpu.VMEM((SLOTS, half, feats), BF16),
        gq=pltpu.VMEM((2, tokens, feats), BF16),
        inv=pltpu.VMEM((tokens, 128), F32),
        actv=pltpu.VMEM((tokens, latents), BF16),
        actt=pltpu.VMEM((latents, tokens), BF16),
        slopes=pltpu.VMEM((tokens, latents), F32),
        lown=pltpu.VMEM((tokens, feats), BF16),
        lpeer=pltpu.VMEM((half, feats), BF16),
        llow=pltpu.VMEM((2, half, feats), BF16),
        sacc=pltpu.VMEM((4, half, feats), F32),
        sout=pltpu.VMEM((3, half, feats), BF16),
        s0in=pltpu.VMEM((tokens, feats), BF16),
        og=pltpu.VMEM((tokens, feats), BF16),
        acc=pltpu.VMEM((4 * MIXES, 8, 128), F32),
        wall=pltpu.VMEM((4, MIXES, 128), F32),
        mst=pltpu.VMEM((4, MIXES, 128), F32),
        mtot=pltpu.VMEM((MIXES, 128), F32),
        mixin=pltpu.VMEM((2, 2, n, MIXES, 128), F32),
        upv=pltpu.VMEM((latents, feats), BF16),
        apown=pltpu.VMEM((tokens, latents), F32),
        apart=pltpu.VMEM((tokens, latents), BF16),
        rsb=pltpu.VMEM((n, tokens, latents), BF16),
        loc=DMA((6,)),
        gsend=DMA((2, chunks)), grecv=DMA((2, chunks)),
        qsend=DMA((2, n)), qrecv=DMA((2, n)),
        xsend=DMA((n,)), xrecv=DMA((n,)),
        tsend=DMA((n,)), trecv=DMA((n,)),
        isend=DMA((n,)), irecv=DMA((n,)),
        wsend=DMA((4,)), wrecv=DMA((4,)),
        zsend=DMA((4, chunks)), zrecv=DMA((SLOTS, chunks)),
        lsend=DMA((n,)), lrecv=DMA((n,)),
        usend=DMA((2, n)), urecv=DMA((2, n)),
        ssend=DMA((3, chunks)), srecv=DMA((3, chunks)),
        rsend=DMA((n, n)), rrecv=DMA((n, n)),
        msend=DMA((2, 2, n)), mrecv=DMA((2, 2, n)),
    )


def exchange(
    n, stride, names,
    x_ref, lat_ref, g_ref, down_ref, up_ref, gain_ref, mw_ref,
    upg_ref, nt_ref, lg_ref, downv, mix_ref,
    *refs,
):
    s = type("Scratch", (), dict(zip(names, refs)))
    xo, cin, latv, gb, gq, inv = s.xo, s.cin, s.latv, s.gb, s.gq, s.inv
    actv, lown, lpeer, llow, sacc, sout = s.actv, s.lown, s.lpeer, s.llow, s.sacc, s.sout
    s0in, og, acc, wall, mst, mtot, mixin, upv = s.s0in, s.og, s.acc, s.wall, s.mst, s.mtot, s.mixin, s.upv
    own_rows, width = x_ref.shape
    feats = width // n
    half = own_rows // 2
    subs = half // CHUNK
    chunks = n * subs
    tiles = feats // TILE

    sec = lax.axis_index("section")
    x = lax.axis_index("dp")
    q = sec // stride
    res = sec % stride
    a = q // 2
    h = q % 2
    o = 1 - h

    def at(level, side):
        return (2 * level + side) * stride + res

    def to(k):
        return lax.rem(x + k, n) if k else x

    def source(k):
        return lax.rem(x + n - k, n) if k else x

    def remote(src, dst, ssem, rsem, section, dp):
        return pltpu.make_async_remote_copy(
            src_ref=src, dst_ref=dst, send_sem=ssem, recv_sem=rsem,
            device_id={"section": section, "dp": dp}, device_id_type=MESH,
        )

    def arrival(dst, rsem):
        return remote(dst, dst, rsem, rsem, at(a, o), x)

    barrier = pltpu.get_barrier_semaphore()

    def greet(section, dp):
        pl.semaphore_signal(
            barrier, inc=1, device_id={"section": section, "dp": dp}, device_id_type=MESH
        )

    for e in range(2):
        for k in range(n):
            if k or e:
                greet(at(a, o if e else h), to(k))

    @pl.when(a == 0)
    def _():
        for e in range(2):
            for k in range(n):
                greet(at(1, o if e else h), to(k))

    @pl.when(a == 1)
    def _():
        for e in range(2):
            for k in range(n):
                greet(at(0, o if e else h), to(k))
        greet(at(2, h), x)

    @pl.when(a == 2)
    def _():
        greet(at(1, h), x)
        greet(at(3, h), x)

    @pl.when(a == 3)
    def _():
        greet(at(2, h), x)

    own_cols = rows(x * feats, feats, 128)
    own_block = rows(x * own_rows, own_rows, own_rows)
    local = [
        pltpu.make_async_copy(x_ref, xo, s.loc.at[0]),
        pltpu.make_async_copy(lat_ref, latv.at[own_block], s.loc.at[1]),
        pltpu.make_async_copy(x_ref.at[:, own_cols], cin.at[own_block], s.loc.at[2]),
        pltpu.make_async_copy(up_ref, upv, s.loc.at[3]),
        pltpu.make_async_copy(down_ref, downv, s.loc.at[4]),
    ]
    for copy in local:
        copy.start()

    def g_local():
        return pltpu.make_async_copy(
            g_ref.at[rows(h * half, half, half), own_cols], gb.at[h, rows(x * half, half, half)], s.loc.at[5]
        )

    def q_local():
        return pltpu.make_async_copy(g_ref.at[:, own_cols], gq.at[h, own_block], s.loc.at[5])

    @pl.when(a > 0)
    def _():
        g_local().start()

    @pl.when(a == 0)
    def _():
        q_local().start()

    @pl.when(h == 0)
    def _():
        for slot in range(MIXES):
            wall[0, slot : slot + 1] = jnp.broadcast_to(mw_ref[0:1, slot : slot + 1], (1, 128))

    @pl.when(h == 1)
    def _():
        wall[0, 0:1] = jnp.zeros((1, 128), F32)
        for slot in range(1, MIXES):
            wall[0, slot : slot + 1] = jnp.broadcast_to(mw_ref[0:1, slot - 1 : slot], (1, 128))

    met = 2 * n - 1 + jnp.where(a < 2, 2 * n, 0) + jnp.where(a == 2, 2, jnp.where(a == 0, 0, 1))
    pl.semaphore_wait(barrier, met)

    sends = {level: [] for level in range(LEVELS)}

    def go(level, make, *args):
        make(*args).start()
        sends[level].append(functools.partial(make, *args))

    def chunk_at(c):
        k, sub = divmod(c, subs)
        return source(k), k, sub

    def span(c):
        j, _, sub = chunk_at(c)
        return rows(j * half + sub * CHUNK, CHUNK, CHUNK)

    def wide(c, side):
        j, _, sub = chunk_at(c)
        return rows(j * own_rows + side * half + sub * CHUNK, CHUNK, CHUNK)

    def g_copy(e, c):
        k, sub = divmod(c, subs)
        side = o if e else h
        return remote(
            g_ref.at[rows(side * half + sub * CHUNK, CHUNK, CHUNK), rows(to(k) * feats, feats, 128)],
            gb.at[h, rows(x * half + sub * CHUNK, CHUNK, CHUNK)],
            s.gsend.at[e, c], s.grecv.at[e, c], at(a, side), to(k),
        )

    def g_wait(e, c):
        arrival(gb.at[o if e else h, span(c)], s.grecv.at[e, c]).wait_recv()

    def q_send(e, k):
        return remote(
            g_ref.at[:, rows(to(k) * feats, feats, 128)], gq.at[h, own_block],
            s.qsend.at[e, k], s.qrecv.at[e, k], at(a, o if e else h), to(k),
        )

    def q_wait(e, k):
        block = rows(source(k) * own_rows, own_rows, own_rows)
        arrival(gq.at[o if e else h, block], s.qrecv.at[e, k]).wait_recv()

    def x_copy(k):
        return remote(
            x_ref.at[:, rows(to(k) * feats, feats, 128)], cin.at[own_block],
            s.xsend.at[k], s.xrecv.at[k], at(a, h), to(k),
        )

    def z_copy(e, c, relay):
        k, sub = divmod(c, subs)
        slot = (o if e else h) + (2 if relay else 0)
        if not relay and not e and not k:
            src = g_ref.at[rows(h * half + sub * CHUNK, CHUNK, CHUNK), own_cols]
        else:
            src = gb.at[slot, span(c)]
        lane = e + (2 if relay else 0)
        return remote(
            src, gb.at[slot + 2, span(c)], s.zsend.at[lane, c], s.zrecv.at[lane + 2, c],
            at(a - 1, h), x,
        )

    def z_wait(e, c, deep):
        slot = (o if e else h) + (4 if deep else 2)
        arrival(gb.at[slot, span(c)], s.zrecv.at[e + (4 if deep else 2), c]).wait_recv()

    def w_copy():
        return remote(wall.at[0], wall.at[1], s.wsend.at[1], s.wrecv.at[1], at(a, o), x)

    def w_low(e):
        return remote(
            wall.at[0], wall.at[2 + e], s.wsend.at[2 + e], s.wrecv.at[2 + e], at(1, o if e else h), x
        )

    def square():
        local[0].wait()

        def step(t, total):
            part = xo[:, rows(t * TILE, TILE, 128)].astype(F32)
            part = part * part
            for at_col in range(0, TILE, 128):
                total = total + part[:, at_col : at_col + 128]
            return total

        lanes = lax.fori_loop(0, width // TILE, step, jnp.zeros((own_rows, 128), F32))
        mean_sq = jnp.sum(lanes, axis=1, keepdims=True) / width
        inv[own_block] = jnp.broadcast_to(lax.rsqrt(mean_sq + epsilon), (own_rows, 128))

    def inv_copy(k):
        return remote(
            inv.at[own_block], inv.at[own_block], s.isend.at[k], s.irecv.at[k], at(a, h), to(k)
        )

    def inv_send(level):
        for k in range(1, n):
            go(level, inv_copy, k)

    def lat_copy(k):
        return remote(
            lat_ref, latv.at[own_block], s.tsend.at[k], s.trecv.at[k], at(a, h), to(k)
        )

    def gelu(k):
        block = rows(source(k) * own_rows, own_rows, own_rows)
        if k:
            arrival(latv.at[block], s.trecv.at[k]).wait_recv()
        else:
            local[1].wait()
        values, slopes = gelu_pair(latv[block].astype(F32))
        actv[block] = values.astype(BF16)
        s.slopes[block] = slopes

    def layer_out(k):
        block = rows(source(k) * own_rows, own_rows, own_rows)
        if k:
            arrival(cin.at[block], s.xrecv.at[k]).wait_recv()
        else:
            local[2].wait()
            local[3].wait()

        @pl.loop(0, tiles)
        def _(t):
            cols = rows(t * TILE, TILE, 128)
            branch = jnp.dot(actv[block, :], upv[:, cols], preferred_element_type=F32)
            lown[block, cols] = (cin[block, cols].astype(F32) + branch).astype(BF16)

    def l_copy(k):
        j = source(k)
        return remote(
            lown.at[rows(j * own_rows + o * half, half, half)], lpeer.at[rows(j * half, half, half)],
            s.lsend.at[k], s.lrecv.at[k], at(a, o), x,
        )

    def l_wait(k):
        arrival(lpeer.at[rows(source(k) * half, half, half)], s.lrecv.at[k]).wait_recv()

    def up_copy(e, k):
        j = source(k)
        block = rows(j * half, half, half)
        src = lpeer.at[block] if e else lown.at[rows(j * own_rows + h * half, half, half)]
        return remote(src, llow.at[e, block], s.usend.at[e, k], s.urecv.at[e, k], at(1, h), x)

    def up_wait(k):
        for e in range(2):
            arrival(llow.at[e, rows(source(k) * half, half, half)], s.urecv.at[e, k]).wait_recv()

    def weight(target, slot):
        slot = slot + 2 if target > 1 else slot
        return wall[target, slot : slot + 1, 0:1]

    def add(c, slots, targets, first, final):
        here = span(c)
        mine = wide(c, h)

        @pl.loop(0, tiles)
        def _(t):
            cols = rows(t * TILE, TILE, 128)
            parts = [gb[slot, here, cols].astype(F32) for slot in slots]
            for target in range(targets):
                value = None if first else sacc[target, here, cols]
                for slot, part in zip(slots, parts):
                    term = weight(target, slot) * part
                    value = term if value is None else value + term
                if not final:
                    sacc[target, here, cols] = value
                elif target == 0:
                    og[mine, cols] = value.astype(BF16)
                else:
                    sout[target - 1, here, cols] = value.astype(BF16)

    def s_copy(c):
        return remote(
            sout.at[0, span(c)], og.at[wide(c, h)], s.ssend.at[0, c], s.srecv.at[0, c], at(a, o), x
        )

    def s0_copy(e, c):
        return remote(
            sout.at[1 + e, span(c)], s0in.at[wide(c, h)], s.ssend.at[1 + e, c], s.srecv.at[1 + e, c],
            at(0, o if e else h), x,
        )

    def s_wait(c):
        arrival(og.at[wide(c, o)], s.srecv.at[0, c]).wait_recv()

    def s0_wait(c):
        for e in range(2):
            arrival(s0in.at[wide(c, o if e else h)], s.srecv.at[1 + e, c]).wait_recv()

    def inner(c, slots, targets):
        here = span(c)
        mine = wide(c, h)

        @pl.loop(0, tiles)
        def _(t):
            cols = rows(t * TILE, TILE, 128)
            parts = [gb[slot, here, cols].astype(F32) for slot in slots]
            for target in range(targets):
                if target == 0:
                    other = lown[mine, cols]
                elif target == 1:
                    other = lpeer[here, cols]
                else:
                    other = llow[target - 2, here, cols]
                other = other.astype(F32)
                for slot, part in zip(slots, parts):
                    place = MIXES * target + (slot + 2 if target > 1 else slot)
                    acc[place] += fold(part * other)

    def mix_parts(targets):
        for target in range(targets):
            for slot in range(MIXES):
                mst[target, slot : slot + 1] = jnp.sum(acc[MIXES * target + slot], axis=0, keepdims=True)

    def mix_copy(target, k):
        low, e = divmod(target, 2)
        return remote(
            mst.at[target], mixin.at[low, e, k], s.msend.at[low, e, k], s.mrecv.at[low, e, k],
            at(0 if low else a, o if e else h), to(k),
        )

    def mix_send(target, level):
        for k in range(n):
            if k or target:
                go(level, mix_copy, target, k)

    def mix_take(low, e):
        for k in range(n):
            if k or low or e:
                arrival(mixin.at[low, e, k], s.mrecv.at[low, e, k]).wait_recv()
                mtot[...] += mixin[low, e, k]

    def act_block(k):
        j = source(k)
        block = rows(j * own_rows, own_rows, own_rows)
        part = lax.dot_general(
            og[block, :], upv[...], (((1,), (1,)), ((), ())), preferred_element_type=F32,
        )
        s.apown[block] = part
        s.apart[block] = part.astype(BF16)

    def act_copy(d, k):
        block = rows(source(k) * own_rows, own_rows, own_rows)
        return remote(
            s.apart.at[block], s.rsb.at[d, block], s.rsend.at[d, k], s.rrecv.at[d, k], at(a, h), to(d)
        )

    def act_send(k, level):
        for d in range(1, n):
            go(level, act_copy, d, k)

    def normed():
        for k in range(1, n):
            block = rows(source(k) * own_rows, own_rows, own_rows)
            arrival(inv.at[block], s.irecv.at[k]).wait_recv()

        @pl.loop(0, tiles)
        def _(t):
            cols = rows(t * TILE, TILE, 128)
            scaled = cin[:, cols].astype(F32) * inv[:, 0:1]
            normed = (scaled * gain_ref[:, cols].astype(F32)).astype(BF16)
            nt_ref[rows(t * TILE, TILE, 128), :] = normed.T

    def begin():
        acc[...] = jnp.zeros_like(acc)
        square()
        gelu(0)

    def middle():
        for k in range(1, n):
            gelu(k)
        s.actt[...] = actv[...].T

    def first_sends(level):
        go(level, w_copy)
        for k in range(1, n):
            go(level, lat_copy, k)

    def w_take():
        arrival(wall.at[1], s.wrecv.at[1]).wait_recv()

    def spread(level, x_first):
        for sub in range(subs):
            go(level, g_copy, 1, sub)
        if x_first:
            for k in range(1, n):
                go(level, x_copy, k)
        for k in range(1, n):
            for e in range(2):
                for sub in range(subs):
                    go(level, g_copy, e, k * subs + sub)
        if not x_first:
            for k in range(1, n):
                go(level, x_copy, k)

    near = (0, 1)

    def own_take(k):
        for sub in range(subs):
            c = k * subs + sub
            for e in range(2):
                if k or e:
                    g_wait(e, c)
        if k == 0:
            g_local().wait()

    @pl.when(a == 3)
    def _():
        L = 3
        for sub in range(subs):
            go(L, z_copy, 0, sub, False)
        first_sends(L)
        spread(L, False)
        begin()
        inv_send(L)
        layer_out(0)
        go(L, l_copy, 0)
        for sub in range(subs):
            g_wait(1, sub)
            go(L, z_copy, 1, sub, False)
        g_local().wait()
        for k in range(1, n):
            for e in range(2):
                for sub in range(subs):
                    g_wait(e, k * subs + sub)
                    go(L, z_copy, e, k * subs + sub, False)
        w_take()
        for c in range(chunks):
            add(c, near, 2, True, True)
            go(L, s_copy, c)
        middle()
        for k in range(1, n):
            layer_out(k)
            go(L, l_copy, k)
        normed()
        for k in range(n):
            l_wait(k)
            for sub in range(subs):
                inner(k * subs + sub, near, 2)
        mix_parts(2)
        mix_send(0, L)
        mix_send(1, L)
        for k in range(n):
            for sub in range(subs):
                s_wait(k * subs + sub)
            act_block(k)
            act_send(k, L)

    @pl.when(a == 2)
    def _():
        L = 2
        for sub in range(subs):
            go(L, z_copy, 0, sub, False)
        first_sends(L)
        spread(L, False)
        begin()
        inv_send(L)
        for sub in range(subs):
            g_wait(1, sub)
            go(L, z_copy, 1, sub, False)
        g_local().wait()
        layer_out(0)
        go(L, l_copy, 0)
        w_take()
        for k in range(1, n):
            for e in range(2):
                for sub in range(subs):
                    g_wait(e, k * subs + sub)
                    go(L, z_copy, e, k * subs + sub, False)
        for k in range(n):
            for sub in range(subs):
                c = k * subs + sub
                for e in range(2):
                    z_wait(e, c, False)
                    go(L, z_copy, e, c, True)
                add(c, (0, 1, 2, 3), 2, True, True)
                go(L, s_copy, c)
        middle()
        for k in range(1, n):
            layer_out(k)
            go(L, l_copy, k)
        normed()
        for k in range(n):
            l_wait(k)
            for sub in range(subs):
                inner(k * subs + sub, (0, 1, 2, 3), 2)
        mix_parts(2)
        mix_send(0, L)
        mix_send(1, L)
        for k in range(n):
            for sub in range(subs):
                s_wait(k * subs + sub)
            act_block(k)
            act_send(k, L)

    @pl.when(a == 1)
    def _():
        L = 1
        first_sends(L)
        spread(L, True)
        begin()
        inv_send(L)
        layer_out(0)
        go(L, l_copy, 0)
        w_take()
        for e in range(2):
            arrival(wall.at[2 + e], s.wrecv.at[2 + e]).wait_recv()
        own_take(0)
        for sub in range(subs):
            add(sub, near, 4, True, False)
        middle()
        for k in range(1, n):
            layer_out(k)
            go(L, l_copy, k)
        for sub in range(subs):
            for e in range(2):
                z_wait(e, sub, False)
            add(sub, (2, 3), 4, False, False)
        normed()
        l_wait(0)
        up_wait(0)
        for sub in range(subs):
            inner(sub, (0, 1, 2, 3), 4)
        for k in range(1, n):
            own_take(k)
            for sub in range(subs):
                c = k * subs + sub
                for e in range(2):
                    z_wait(e, c, False)
                add(c, (0, 1, 2, 3), 4, True, False)
        todo = []
        for c in range(chunks):
            for e in range(2):
                z_wait(e, c, True)
            add(c, (4, 5), 4, False, True)
            for e in range(2):
                go(L, s0_copy, e, c)
            go(L, s_copy, c)
            k, sub = divmod(c, subs)
            if k and sub == 0:
                for s2 in range(subs):
                    s_wait((k - 1) * subs + s2)
                act_block(k - 1)
                act_send(k - 1, L)
            if k and sub == subs - 2:
                l_wait(k)
                up_wait(k)
                for late in todo:
                    inner(late, (0, 1, 2, 3, 4, 5), 4)
                todo = []
            if k == 0:
                inner(c, (4, 5), 4)
            elif sub >= subs - 2:
                inner(c, (0, 1, 2, 3, 4, 5), 4)
            else:
                todo.append(c)
        mix_parts(4)
        for target in range(4):
            mix_send(target, L)
        k = n - 1
        for sub in range(subs):
            s_wait(k * subs + sub)
        act_block(k)
        act_send(k, L)

    @pl.when(a == 0)
    def _():
        L = 0
        first_sends(L)
        for e in range(2):
            go(L, w_low, e)

        @pl.when(h == 1)
        def _():
            q_send(1, 0).start()

        for k in range(1, n):
            go(L, x_copy, k)
        for k in range(1, n):
            go(L, q_send, 0, k)
        begin()
        inv_send(L)
        layer_out(0)
        go(L, l_copy, 0)
        go(L, up_copy, 0, 0)

        @pl.when(h == 1)
        def _():
            for k in range(1, n):
                q_send(1, k).start()

        w_take()
        middle()
        l_wait(0)
        go(L, up_copy, 1, 0)
        for k in range(1, n):
            layer_out(k)
            go(L, l_copy, k)
            go(L, up_copy, 0, k)
            l_wait(k)
            go(L, up_copy, 1, k)
        normed()
        q_local().wait()
        for k in range(1, n):
            q_wait(0, k)

        @pl.when(h == 0)
        def _():
            for k in range(n):
                q_wait(1, k)

        def whole_inner(slot):
            @pl.loop(0, n * own_rows // CHUNK)
            def _(c):
                here = rows(c * CHUNK, CHUNK, CHUNK)

                @pl.loop(0, tiles)
                def _(t):
                    cols = rows(t * TILE, TILE, 128)
                    acc[slot] += fold(gq[slot, here, cols].astype(F32) * lown[here, cols].astype(F32))

        whole_inner(1)

        @pl.when(h == 0)
        def _():
            whole_inner(0)

        mix_parts(1)
        mix_send(0, L)

        def finish(c, slots):
            @pl.loop(0, tiles)
            def _(t):
                cols = rows(t * TILE, TILE, 128)
                for side in (h, o):
                    here = wide(c, side)
                    value = s0in[here, cols].astype(F32)
                    for slot in slots:
                        value = value + weight(0, slot) * gq[slot, here, cols].astype(F32)
                    og[here, cols] = value.astype(BF16)

        for c in range(chunks):
            s0_wait(c)

            @pl.when(h == 0)
            def _():
                finish(c, (0, 1))

            @pl.when(h == 1)
            def _():
                finish(c, (1,))

            k, sub = divmod(c, subs)
            if sub == subs - 1:
                act_block(k)
                act_send(k, L)

    @pl.loop(0, tiles)
    def _(t):
        cols = rows(t * TILE, TILE, 128)
        upg_ref[:, cols] = jnp.dot(s.actt[...], og[:, cols], preferred_element_type=F32).astype(BF16)

    mtot[...] = mst[0]

    @pl.when(a > 0)
    def _():
        mix_take(0, 0)
        mix_take(0, 1)

    @pl.when(a == 0)
    def _():
        mix_take(0, 0)
        mix_take(1, 0)
        mix_take(1, 1)

    sums = jnp.sum(mtot[...], axis=1, keepdims=True)
    lane = lax.broadcasted_iota(jnp.int32, (1, MIXES), 1)

    def mix_row(shift):
        row = jnp.zeros((1, MIXES), F32)
        for m in range(MIXES - shift):
            row = jnp.where(lane == m, sums[m + shift : m + shift + 1, 0:1], row)
        mix_ref[...] = row

    @pl.when(h == 0)
    def _():
        mix_row(0)

    @pl.when(h == 1)
    def _():
        mix_row(1)

    local[4].wait()
    for k in range(n):
        block = rows(source(k) * own_rows, own_rows, own_rows)
        total = s.apown[block]
        for d in range(1, n):
            arrival(s.rsb.at[d, block], s.rrecv.at[d, (k - d) % n]).wait_recv()
            total = total + s.rsb[d, block].astype(F32)
        lg_ref[block] = (total * s.slopes[block]).astype(BF16)

    for level in range(LEVELS):
        @pl.when(a == level)
        def _():
            for make in sends[level]:
                make().wait_send()

    @pl.when(jnp.logical_and(a == 0, h == 1))
    def _():
        for k in range(n):
            q_send(1, k).wait_send()


def finish(
    upg_ref, nt_ref, lg_ref, down_ref, mix_ref, gain_ref,
    upo_ref, dno_ref, gaino_ref, mixo_ref, dn, sems,
):
    feats, latents = down_ref.shape
    out = [pltpu.make_async_copy(upg_ref, upo_ref, sems.at[0])]
    out[0].start()
    mixo_ref[...] = mix_ref[...]
    for t in range(feats // TILE):
        here = slice(t * TILE, (t + 1) * TILE)
        grad = jnp.dot(nt_ref[here, :], lg_ref[...], preferred_element_type=F32)
        dn[here, :] = grad.astype(BF16)
        copy = pltpu.make_async_copy(dn.at[here], dno_ref.at[here], sems.at[1 + t])
        copy.start()
        out.append(copy)
        prod = grad * down_ref[here, :].astype(F32)
        lanes = prod[:, 0:128]
        for at in range(128, latents, 128):
            lanes = lanes + prod[:, at : at + 128]
        for b in range(TILE // 128):
            cols = slice(t * TILE + b * 128, t * TILE + (b + 1) * 128)
            row = jnp.sum(lanes[b * 128 : (b + 1) * 128, :].T, axis=0, keepdims=True)
            gaino_ref[:, cols] = row / gain_ref[:, cols].astype(F32)
    for copy in out:
        copy.wait()


def local(layer_in, latent, mix_grad, down_proj, up_proj, norm_gain, mix_weight):
    _, own_rows, width = layer_in.shape
    n = lax.axis_size("dp")
    stride = lax.axis_size("section") // MIXES
    latents = latent.shape[2]
    feats = width // n
    tokens = own_rows * n
    anyspace = pl.BlockSpec(memory_space=pl.ANY)
    vmem = pl.BlockSpec(memory_space=pltpu.VMEM)
    space = scratch(n, own_rows, width, latents)
    held = pl.pallas_call(
        functools.partial(exchange, n, stride, tuple(space)),
        out_shape=(
            pltpu.VMEM((latents, feats), BF16),
            pltpu.VMEM((feats, tokens), BF16),
            pltpu.VMEM((tokens, latents), BF16),
            pltpu.VMEM((feats, latents), BF16),
            pltpu.VMEM((1, MIXES), F32),
        ),
        in_specs=[anyspace] * 5 + [vmem] * 2,
        out_specs=(vmem,) * 5,
        scratch_shapes=list(space.values()),
        compiler_params=pltpu.CompilerParams(
            collective_id=0, has_side_effects=True, vmem_limit_bytes=48 * 1024 * 1024
        ),
        name="exchange",
    )(layer_in[0], latent[0], mix_grad[0], down_proj[0], up_proj[0], norm_gain, mix_weight)
    up_grad, down_grad, gain_grad, mixed = pl.pallas_call(
        finish,
        out_shape=(
            jax.ShapeDtypeStruct((latents, feats), BF16),
            jax.ShapeDtypeStruct((feats, latents), BF16),
            jax.ShapeDtypeStruct((1, feats), F32),
            jax.ShapeDtypeStruct((1, MIXES), F32),
        ),
        in_specs=[vmem] * 6,
        out_specs=(anyspace, anyspace, vmem, vmem),
        scratch_shapes=[pltpu.VMEM((feats, latents), BF16), DMA((1 + feats // TILE,))],
        compiler_params=pltpu.CompilerParams(vmem_limit_bytes=12 * 1024 * 1024),
        name="finish",
    )(*held, norm_gain)
    return (up_grad[None], down_grad[None], gain_grad, mixed)


def solution(mesh):
    return jax.shard_map(
        local,
        mesh=mesh,
        in_specs=(
            P("section", "dp", None),
            P("section", "dp", None),
            P("section", "dp", None),
            P("section", "dp", None),
            P("section", None, "dp"),
            P("section", "dp"),
            P("section", None),
        ),
        out_specs=(
            P("section", None, "dp"),
            P("section", "dp", None),
            P("section", "dp"),
            P("section", None),
        ),
        check_vma=False,
    )
```
